32 devices in a mesh: row: 8 (over y, x, core), col: 4 (over z).
Axes of the slice: x: 2, y: 2, z: 4, core: 2. Of those that a mesh axis runs over, the one named last changes fastest.
Arguments:
- adjacency: int32 [2560, 80], P('row', 'col'), may hold values from -2147483648 to 2147483647, as said below
- relabel: int32 [2560], P(('row', 'col')), may hold values from 0 to 2559, each once
Outputs:
- clustering: float32 [2560], P(('row', 'col'))
- transitivity: float32 [], replicated
The draws below stay inside these ranges and needn't reach their ends.
Inputs may be any that keep to these rules, and one draw needn't show every extreme that they name: The unpacked adjacency is symmetric with a zero diagonal.
All inputs are finite; a program needn't handle non-finite values.
Results may differ from the reference program's by a relative error of at most 0.0003.
Values sent between devices are 32-bit elements.
A program may use at most 128 MiB of HBM per device.

```python
import jax
import jax.numpy as jnp
from jax import lax

NV = 2560
N_ROW = 8


def draw_adjacency(key, part):
    first, second = jax.random.split(jax.random.fold_in(key, 23), 2)
    activity = jax.random.randint(first, (NV,), 1, 5)
    thresh = 1000 * activity[:, None] * activity[None, :]
    coins = jax.random.randint(second, (NV, NV), 0, 65536)
    keep = coins < thresh
    index = jnp.arange(NV)
    upper = keep & (index[None, :] > index[:, None])
    links = (upper | upper.T).astype(jnp.int32)
    bits = links.reshape(NV, NV // 32, 32)
    shifts = jnp.arange(32, dtype=jnp.int32)
    words = jnp.sum(lax.shift_left(bits, shifts[None, None, :]), axis=2)
    return words.astype(jnp.int32)


def setup_inputs(seed: int = 0) -> dict:
    key_list = jax.random.split(jax.random.key(seed), 3)
    return {
        "adjacency": draw_adjacency(jax.random.fold_in(key_list[2], 71), 0),
        "relabel": jax.random.permutation(key_list[1], NV).astype(jnp.int32),
    }


def unpack(words):
    shifts = jnp.arange(32, dtype=jnp.int32)
    bits = lax.shift_right_logical(words[:, :, None], shifts[None, None, :]) & 1
    return bits.reshape(words.shape[0], words.shape[1] * 32).astype(jnp.bfloat16)


def reference(adjacency, relabel):
    links = unpack(adjacency)
    block_rows = NV // N_ROW
    starts = jnp.arange(N_ROW, dtype=jnp.int32) * block_rows

    def one_block(offset):
        rows = lax.dynamic_slice_in_dim(links, offset.astype(jnp.int32), block_rows, 0)
        paths = jnp.dot(rows, links, preferred_element_type=jnp.float32)
        wide = rows.astype(jnp.float32)
        return jnp.sum(wide * paths, axis=1), jnp.sum(wide, axis=1)

    closed, degree = lax.map(one_block, starts)
    closed = closed.reshape(NV)
    degree = degree.reshape(NV)
    wedges = jnp.maximum(degree * (degree - 1.0), 1.0)
    ratio = closed / wedges
    clustering = jnp.take(ratio, relabel, axis=0)
    transitivity = jnp.sum(closed) / jnp.sum(wedges)
    return clustering, transitivity
```

```python
import functools

import jax
import jax.numpy as jnp
from jax import lax
from jax.experimental import pallas as pl
from jax.experimental.pallas import tpu as pltpu
from jax.sharding import PartitionSpec as P

MESH = pl.DeviceIdType.MESH
TYPE = jnp.float8_e4m3fn


def unpack(row):
    wide = jnp.broadcast_to(row, (32, row.shape[1]))
    bits = lax.shift_right_logical(wide, lax.broadcasted_iota(jnp.int32, wide.shape, 0)) & 1
    return bits.astype(jnp.float32).astype(TYPE)


def kernel(
    n_row, n_col, words_ref, relabel_ref, out_ref, total_ref,
    xs, ys, yw, x, y, hot, rel, msg,
    x_send, x_recv, y_send, y_recv, m_send, m_recv, local_sem,
):
    n_words, n_rows = words_ref.shape
    n_mine = relabel_ref.shape[1]
    depth = 32 * n_words
    width = msg.shape[1]
    r, c = lax.axis_index("row"), lax.axis_index("col")
    barrier = pltpu.get_barrier_semaphore()
    col_peers = [lax.rem(c + o, n_col) for o in range(1, n_col)]
    row_peers = [lax.rem(r + o, n_row) for o in range(1, n_row)]
    for p in col_peers:
        pl.semaphore_signal(barrier, inc=1, device_id=(r, p), device_id_type=MESH)
    for p in row_peers:
        pl.semaphore_signal(barrier, inc=1, device_id=(p, c), device_id_type=MESH)
    load_x = pltpu.make_async_copy(words_ref, xs.at[c], local_sem.at[0])
    load_y = pltpu.make_async_copy(words_ref, ys.at[r], local_sem.at[1])
    load_r = pltpu.make_async_copy(relabel_ref, rel, local_sem.at[2])
    load_x.start()
    load_y.start()
    load_r.start()
    load_x.wait()
    load_y.wait()
    pl.semaphore_wait(barrier, n_col + n_row - 2)

    sends = []
    for i, p in enumerate(col_peers):
        sends.append(pltpu.make_async_remote_copy(
            xs.at[c], xs.at[c], x_send.at[i], x_recv.at[c], device_id=(r, p), device_id_type=MESH))
    for i, p in enumerate(row_peers):
        sends.append(pltpu.make_async_remote_copy(
            ys.at[r], ys.at[r], y_send.at[i], y_recv.at[r], device_id=(p, c), device_id_type=MESH))
    for copy in sends:
        copy.start()

    load_r.wait()
    label = rel[...]
    owner = jnp.zeros_like(label)
    for k in range(1, n_row):
        owner += (label >= k * n_rows).astype(jnp.int32)
    place = label - owner * n_rows
    hot[...] = (lax.broadcasted_iota(jnp.int32, hot.shape, 0) == place).astype(jnp.float32).astype(jnp.bfloat16)
    y[depth:, :] = jnp.ones((y.shape[0] - depth, y.shape[1]), TYPE)

    def take_x(block):
        def one(w, carry):
            start = pl.multiple_of(block * depth + w * 32, 32)
            x[pl.ds(start, 32), :] = unpack(xs[block, pl.ds(w, 1), :])
            return carry
        lax.fori_loop(0, n_words, one, 0, unroll=4)

    take_x(c)
    for i, p in enumerate(col_peers):
        pltpu.make_async_remote_copy(
            xs.at[p], xs.at[p], x_send.at[i], x_recv.at[p], device_id=(r, p), device_id_type=MESH).wait_recv()
        take_x(p)
    for i, p in enumerate(row_peers):
        pltpu.make_async_remote_copy(
            ys.at[p], ys.at[p], y_send.at[i], y_recv.at[p], device_id=(p, c), device_id_type=MESH).wait_recv()
    yw[...] = jnp.concatenate([ys[k] for k in range(n_row)], axis=1)

    def one_y(w, carry):
        y[pl.ds(pl.multiple_of(w * 32, 32), 32), :] = unpack(yw[pl.ds(w, 1), :])
        return carry
    lax.fori_loop(0, n_words, one_y, 0, unroll=2)

    paths = jnp.dot(y[...], x[...], preferred_element_type=jnp.float32)
    mask = x[pl.ds(pl.multiple_of(c * depth, 32), depth), :].astype(jnp.float32)
    closed = jnp.sum(paths[:depth] * mask, axis=0, keepdims=True)
    degree = paths[depth : depth + 1]
    wedges = jnp.maximum(degree * (degree - 1.0), 1.0)
    sums = lax.broadcasted_iota(jnp.int32, (1, width - n_rows), 1)
    tail = jnp.where(sums == 0, jnp.sum(closed), jnp.where(sums == 1, jnp.sum(wedges), 0.0))
    me = c * n_row + r
    msg[pl.ds(me, 1), :] = jnp.concatenate([closed / wedges, tail], axis=1)

    posts = []
    i = 0
    for oc in reversed(range(n_col)):
        for orow in range(n_row):
            if oc == 0 and orow == 0:
                continue
            posts.append(pltpu.make_async_remote_copy(
                msg.at[pl.ds(me, 1)], msg.at[pl.ds(me, 1)], m_send.at[i], m_recv.at[me],
                device_id=(lax.rem(r + orow, n_row), lax.rem(c + oc, n_col)), device_id_type=MESH))
            i += 1
    for copy in posts:
        copy.start()
    for copy in sends:
        copy.wait_send()
    for o in range(1, n_row * n_col):
        p = lax.rem(me + o, n_row * n_col)
        pltpu.make_async_copy(msg.at[pl.ds(p, 1)], msg.at[pl.ds(p, 1)], m_recv.at[p]).wait()

    ratio = msg[0:n_row, :]
    for k in range(1, n_col):
        ratio += msg[k * n_row : (k + 1) * n_row, :]
    high = ratio.astype(jnp.bfloat16)
    rest = ratio - high.astype(jnp.float32)
    middle = rest.astype(jnp.bfloat16)
    low = (rest - middle.astype(jnp.float32)).astype(jnp.bfloat16)
    found = jnp.zeros((n_row, n_mine), jnp.float32)
    for part in (high, middle, low):
        found += jnp.dot(part, hot[...], preferred_element_type=jnp.float32)
    which = lax.broadcasted_iota(jnp.int32, found.shape, 0)
    out_ref[...] = jnp.sum(jnp.where(which == owner, found, 0.0), axis=0, keepdims=True)
    sum_closed = jnp.sum(ratio[:, n_rows : n_rows + 1], axis=0, keepdims=True)
    sum_wedges = jnp.sum(ratio[:, n_rows + 1 : n_rows + 2], axis=0, keepdims=True)
    total_ref[...] = sum_closed / (sum_wedges * (1.0 / n_col))
    for copy in posts:
        copy.wait_send()


def solution(mesh):
    n_row, n_col = mesh.shape["row"], mesh.shape["col"]
    n_all = n_row * n_col

    def body(adjacency, relabel):
        n_rows, n_words = adjacency.shape
        n_mine = relabel.shape[0]
        depth = 32 * n_words
        every = n_row * n_rows
        width = (n_rows + 2 + 127) // 128 * 128
        clustering, total = pl.pallas_call(
            functools.partial(kernel, n_row, n_col),
            out_shape=(
                jax.ShapeDtypeStruct((1, n_mine), jnp.float32),
                jax.ShapeDtypeStruct((1, 1), jnp.float32),
            ),
            in_specs=[pl.BlockSpec(memory_space=pl.ANY)] * 2,
            out_specs=[pl.BlockSpec(memory_space=pltpu.VMEM)] * 2,
            scratch_shapes=[
                pltpu.VMEM((n_col, n_words, n_rows), jnp.int32),
                pltpu.VMEM((n_row, n_words, n_rows), jnp.int32),
                pltpu.VMEM((n_words, every), jnp.int32),
                pltpu.VMEM((every, n_rows), TYPE),
                pltpu.VMEM((depth + 32, every), TYPE),
                pltpu.VMEM((width, n_mine), jnp.bfloat16),
                pltpu.VMEM((1, n_mine), jnp.int32),
                pltpu.VMEM((n_all, width), jnp.float32),
                pltpu.SemaphoreType.DMA((n_col - 1,)),
                pltpu.SemaphoreType.DMA((n_col,)),
                pltpu.SemaphoreType.DMA((n_row - 1,)),
                pltpu.SemaphoreType.DMA((n_row,)),
                pltpu.SemaphoreType.DMA((n_all - 1,)),
                pltpu.SemaphoreType.DMA((n_all,)),
                pltpu.SemaphoreType.DMA((3,)),
            ],
            compiler_params=pltpu.CompilerParams(
                collective_id=0, has_side_effects=True, vmem_limit_bytes=64000 * 1024
            ),
        )(adjacency.T, relabel.reshape(1, n_mine))
        return clustering.reshape(n_mine), total.reshape(())

    placed = (P("row", "col"), P(("row", "col")))
    return jax.shard_map(
        body, mesh=mesh, in_specs=placed, out_specs=(P(("row", "col")), P()), check_vma=False
    )
```

```python
import functools

import jax
import jax.numpy as jnp
from jax import lax
from jax.experimental import pallas as pl
from jax.experimental.pallas import tpu as pltpu
from jax.sharding import PartitionSpec as P

MESH = pl.DeviceIdType.MESH
TYPE = jnp.float8_e4m3fn


def unpack(row):
    wide = jnp.broadcast_to(row, (32, row.shape[1]))
    bits = lax.shift_right_logical(wide, lax.broadcasted_iota(jnp.int32, wide.shape, 0)) & 1
    return bits.astype(jnp.float32).astype(TYPE)


def kernel(
    n_row, n_col, words_ref, relabel_ref, out_ref, total_ref,
    xs, ys, yw, x, y, hot, rel, msg,
    x_send, x_recv, y_send, y_recv, m_send, m_recv, local_sem, ready, plane,
):
    n_words, n_rows = words_ref.shape
    n_mine = relabel_ref.shape[1]
    depth = 32 * n_words
    width = msg.shape[1]
    r, c = lax.axis_index("row"), lax.axis_index("col")
    barrier = pltpu.get_barrier_semaphore()

    def each_col(do, when):
        for p in range(n_col):
            pl.when(when(p, c))(functools.partial(do, p))

    def each_row(do, when):
        for p in range(n_row):
            pl.when(when(p, r))(functools.partial(do, p))

    above, below, other = (lambda p, q: p > q), (lambda p, q: p < q), (lambda p, q: p != q)

    def tell(sem, device):
        pl.semaphore_signal(sem, inc=1, device_id=device, device_id_type=MESH)

    each_col(lambda p: tell(barrier, (r, p)), above)
    each_row(lambda p: tell(barrier, (p, c)), above)
    load_x = pltpu.make_async_copy(words_ref, xs.at[c], local_sem.at[0])
    load_y = pltpu.make_async_copy(words_ref, ys.at[r], local_sem.at[1])
    load_r = pltpu.make_async_copy(relabel_ref, rel, local_sem.at[2])
    load_x.start()
    load_y.start()
    load_r.start()

    @pl.when(c + r > 0)
    def _():
        pl.semaphore_wait(barrier, c + r)

    each_col(lambda p: tell(ready.at[c], (r, p)), below)
    each_row(lambda p: tell(ready.at[n_col + r], (p, c)), below)

    def post_x(p):
        return pltpu.make_async_remote_copy(
            xs.at[c], xs.at[c], x_send.at[p], x_recv.at[c], device_id=(r, p), device_id_type=MESH)

    def post_y(p):
        return pltpu.make_async_remote_copy(
            ys.at[r], ys.at[r], y_send.at[p], y_recv.at[r], device_id=(p, c), device_id_type=MESH)

    load_x.wait()
    each_col(lambda p: post_x(p).start(), below)
    load_y.wait()
    each_row(lambda p: post_y(p).start(), below)

    load_r.wait()
    label = rel[...]
    owner = jnp.zeros_like(label)
    for k in range(1, n_row):
        owner += (label >= k * n_rows).astype(jnp.int32)
    place = label - owner * n_rows
    hot[...] = (lax.broadcasted_iota(jnp.int32, hot.shape, 0) == place).astype(jnp.float32).astype(jnp.bfloat16)
    y[depth:, :] = jnp.ones((y.shape[0] - depth, y.shape[1]), TYPE)

    def take_x(block):
        def one(w, carry):
            start = pl.multiple_of(block * depth + w * 32, 32)
            x[pl.ds(start, 32), :] = unpack(xs[block, pl.ds(w, 1), :])
            return carry
        lax.fori_loop(0, n_words, one, 0, unroll=4)

    take_x(c)

    def up_x(p):
        pl.semaphore_wait(ready.at[p], 1)
        post_x(p).start()

    def up_y(p):
        pl.semaphore_wait(ready.at[n_col + p], 1)
        post_y(p).start()

    each_col(up_x, above)
    each_row(up_y, above)
    each_col(lambda p: tell(plane, (r, p)), other)

    for o in range(1, n_col):
        p = lax.rem(c + o, n_col)
        pltpu.make_async_copy(xs.at[p], xs.at[p], x_recv.at[p]).wait()
        take_x(p)
    for o in range(1, n_row):
        p = lax.rem(r + o, n_row)
        pltpu.make_async_copy(ys.at[p], ys.at[p], y_recv.at[p]).wait()
    yw[...] = jnp.concatenate([ys[k] for k in range(n_row)], axis=1)

    def one_y(w, carry):
        y[pl.ds(pl.multiple_of(w * 32, 32), 32), :] = unpack(yw[pl.ds(w, 1), :])
        return carry
    lax.fori_loop(0, n_words, one_y, 0, unroll=2)

    paths = jnp.dot(y[...], x[...], preferred_element_type=jnp.float32)
    mask = x[pl.ds(pl.multiple_of(c * depth, 32), depth), :].astype(jnp.float32)
    closed = jnp.sum(paths[:depth] * mask, axis=0, keepdims=True)
    degree = paths[depth : depth + 1]
    wedges = jnp.maximum(degree * (degree - 1.0), 1.0)
    sums = lax.broadcasted_iota(jnp.int32, (1, width - n_rows), 1)
    tail = jnp.where(sums == 0, jnp.sum(closed), jnp.where(sums == 1, jnp.sum(wedges), 0.0))
    me = c * n_row + r
    msg[pl.ds(me, 1), :] = jnp.concatenate([closed / wedges, tail], axis=1)

    posts = []
    i = 0
    for oc in reversed(range(n_col)):
        for orow in range(n_row):
            if oc == 0 and orow == 0:
                continue
            posts.append(pltpu.make_async_remote_copy(
                msg.at[pl.ds(me, 1)], msg.at[pl.ds(me, 1)], m_send.at[i], m_recv.at[me],
                device_id=(lax.rem(r + orow, n_row), lax.rem(c + oc, n_col)), device_id_type=MESH))
            i += 1
    pl.semaphore_wait(plane, n_col - 1)
    for copy in posts:
        copy.start()
    each_col(lambda p: post_x(p).wait_send(), other)
    each_row(lambda p: post_y(p).wait_send(), other)
    for o in range(1, n_row * n_col):
        p = lax.rem(me + o, n_row * n_col)
        pltpu.make_async_copy(msg.at[pl.ds(p, 1)], msg.at[pl.ds(p, 1)], m_recv.at[p]).wait()

    ratio = msg[0:n_row, :]
    for k in range(1, n_col):
        ratio += msg[k * n_row : (k + 1) * n_row, :]
    high = ratio.astype(jnp.bfloat16)
    rest = ratio - high.astype(jnp.float32)
    middle = rest.astype(jnp.bfloat16)
    low = (rest - middle.astype(jnp.float32)).astype(jnp.bfloat16)
    found = jnp.zeros((n_row, n_mine), jnp.float32)
    for part in (high, middle, low):
        found += jnp.dot(part, hot[...], preferred_element_type=jnp.float32)
    which = lax.broadcasted_iota(jnp.int32, found.shape, 0)
    out_ref[...] = jnp.sum(jnp.where(which == owner, found, 0.0), axis=0, keepdims=True)
    sum_closed = jnp.sum(ratio[:, n_rows : n_rows + 1], axis=0, keepdims=True)
    sum_wedges = jnp.sum(ratio[:, n_rows + 1 : n_rows + 2], axis=0, keepdims=True)
    total_ref[...] = sum_closed / (sum_wedges * (1.0 / n_col))
    for copy in posts:
        copy.wait_send()


def solution(mesh):
    n_row, n_col = mesh.shape["row"], mesh.shape["col"]
    n_all = n_row * n_col

    def body(adjacency, relabel):
        n_rows, n_words = adjacency.shape
        n_mine = relabel.shape[0]
        depth = 32 * n_words
        every = n_row * n_rows
        width = (n_rows + 2 + 127) // 128 * 128
        clustering, total = pl.pallas_call(
            functools.partial(kernel, n_row, n_col),
            out_shape=(
                jax.ShapeDtypeStruct((1, n_mine), jnp.float32),
                jax.ShapeDtypeStruct((1, 1), jnp.float32),
            ),
            in_specs=[pl.BlockSpec(memory_space=pl.ANY)] * 2,
            out_specs=[pl.BlockSpec(memory_space=pltpu.VMEM)] * 2,
            scratch_shapes=[
                pltpu.VMEM((n_col, n_words, n_rows), jnp.int32),
                pltpu.VMEM((n_row, n_words, n_rows), jnp.int32),
                pltpu.VMEM((n_words, every), jnp.int32),
                pltpu.VMEM((every, n_rows), TYPE),
                pltpu.VMEM((depth + 32, every), TYPE),
                pltpu.VMEM((width, n_mine), jnp.bfloat16),
                pltpu.VMEM((1, n_mine), jnp.int32),
                pltpu.VMEM((n_all, width), jnp.float32),
                pltpu.SemaphoreType.DMA((n_col,)),
                pltpu.SemaphoreType.DMA((n_col,)),
                pltpu.SemaphoreType.DMA((n_row,)),
                pltpu.SemaphoreType.DMA((n_row,)),
                pltpu.SemaphoreType.DMA((n_all - 1,)),
                pltpu.SemaphoreType.DMA((n_all,)),
                pltpu.SemaphoreType.DMA((3,)),
                pltpu.SemaphoreType.REGULAR((n_col + n_row,)),
                pltpu.SemaphoreType.REGULAR,
            ],
            compiler_params=pltpu.CompilerParams(
                collective_id=0, has_side_effects=True, vmem_limit_bytes=64000 * 1024
            ),
        )(adjacency.T, relabel.reshape(1, n_mine))
        return clustering.reshape(n_mine), total.reshape(())

    placed = (P("row", "col"), P(("row", "col")))
    return jax.shard_map(
        body, mesh=mesh, in_specs=placed, out_specs=(P(("row", "col")), P()), check_vma=False
    )
```

```python
import functools

import jax
import jax.numpy as jnp
from jax import lax
from jax.experimental import pallas as pl
from jax.experimental.pallas import tpu as pltpu
from jax.sharding import PartitionSpec as P

MESH = pl.DeviceIdType.MESH
TYPE = jnp.float8_e4m3fn


def unpack(row):
    wide = jnp.broadcast_to(row, (32, row.shape[1]))
    bits = lax.shift_right_logical(wide, lax.broadcasted_iota(jnp.int32, wide.shape, 0)) & 1
    return bits.astype(jnp.float32).astype(TYPE)


def kernel(
    n_row, n_col, words_ref, relabel_ref, out_ref, total_ref,
    xs, ys, yw, x, y, hot, rel, msg,
    x_send, x_recv, y_send, y_recv, m_send, m_recv, local_sem,
):
    n_words, n_rows = words_ref.shape
    n_mine = relabel_ref.shape[1]
    depth = 32 * n_words
    width = msg.shape[1]
    r, c = lax.axis_index("row"), lax.axis_index("col")
    barrier = pltpu.get_barrier_semaphore()
    col_peers = [lax.rem(c + o, n_col) for o in range(1, n_col)]
    row_peers = [lax.rem(r + o, n_row) for o in range(1, n_row)]
    for p in col_peers:
        pl.semaphore_signal(barrier, inc=1, device_id=(r, p), device_id_type=MESH)
    for p in row_peers:
        pl.semaphore_signal(barrier, inc=1, device_id=(p, c), device_id_type=MESH)
    load_x = pltpu.make_async_copy(words_ref, xs.at[c], local_sem.at[0])
    load_y = pltpu.make_async_copy(words_ref, ys.at[r], local_sem.at[1])
    load_r = pltpu.make_async_copy(relabel_ref, rel, local_sem.at[2])
    load_x.start()
    load_y.start()
    load_r.start()
    load_x.wait()
    load_y.wait()
    pl.semaphore_wait(barrier, n_col + n_row - 2)

    sends = []
    for i, p in enumerate(col_peers):
        sends.append(pltpu.make_async_remote_copy(
            xs.at[c], xs.at[c], x_send.at[i], x_recv.at[c], device_id=(r, p), device_id_type=MESH))
    for i, p in enumerate(row_peers):
        sends.append(pltpu.make_async_remote_copy(
            ys.at[r], ys.at[r], y_send.at[i], y_recv.at[r], device_id=(p, c), device_id_type=MESH))
    for copy in sends:
        copy.start()

    load_r.wait()
    label = rel[...]
    owner = jnp.zeros_like(label)
    for k in range(1, n_row):
        owner += (label >= k * n_rows).astype(jnp.int32)
    place = label - owner * n_rows
    hot[...] = (lax.broadcasted_iota(jnp.int32, hot.shape, 0) == place).astype(jnp.float32).astype(jnp.bfloat16)
    y[depth:, :] = jnp.ones((y.shape[0] - depth, y.shape[1]), TYPE)

    def take_x(block):
        def one(w, carry):
            start = pl.multiple_of(block * depth + w * 32, 32)
            x[pl.ds(start, 32), :] = unpack(xs[block, pl.ds(w, 1), :])
            return carry
        lax.fori_loop(0, n_words, one, 0, unroll=4)

    take_x(c)
    for i, p in enumerate(col_peers):
        pltpu.make_async_remote_copy(
            xs.at[p], xs.at[p], x_send.at[i], x_recv.at[p], device_id=(r, p), device_id_type=MESH).wait_recv()
        take_x(p)
    for i, p in enumerate(row_peers):
        pltpu.make_async_remote_copy(
            ys.at[p], ys.at[p], y_send.at[i], y_recv.at[p], device_id=(p, c), device_id_type=MESH).wait_recv()
    yw[...] = jnp.concatenate([ys[k] for k in range(n_row)], axis=1)

    def one_y(w, carry):
        y[pl.ds(pl.multiple_of(w * 32, 32), 32), :] = unpack(yw[pl.ds(w, 1), :])
        return carry
    lax.fori_loop(0, n_words, one_y, 0, unroll=2)

    paths = jnp.dot(y[...], x[...], preferred_element_type=jnp.float32)
    mask = x[pl.ds(pl.multiple_of(c * depth, 32), depth), :].astype(jnp.float32)
    closed = jnp.sum(paths[:depth] * mask, axis=0, keepdims=True)
    degree = paths[depth : depth + 1]
    wedges = jnp.maximum(degree * (degree - 1.0), 1.0)
    sums = lax.broadcasted_iota(jnp.int32, (1, width - n_rows), 1)
    tail = jnp.where(sums == 0, jnp.sum(closed), jnp.where(sums == 1, jnp.sum(wedges), 0.0))
    me = c * n_row + r
    msg[pl.ds(me, 1), :] = jnp.concatenate([closed / wedges, tail], axis=1)

    posts = []
    for i in range(n_row * n_col - 1):
        to = i + (i >= me).astype(jnp.int32)
        posts.append(pltpu.make_async_remote_copy(
            msg.at[pl.ds(me, 1)], msg.at[pl.ds(me, 1)], m_send.at[i], m_recv.at[me],
            device_id=(lax.rem(to, n_row), to // n_row), device_id_type=MESH))
    for copy in posts:
        copy.start()
    for copy in sends:
        copy.wait_send()
    for o in range(1, n_row * n_col):
        p = lax.rem(me + o, n_row * n_col)
        pltpu.make_async_copy(msg.at[pl.ds(p, 1)], msg.at[pl.ds(p, 1)], m_recv.at[p]).wait()

    ratio = msg[0:n_row, :]
    for k in range(1, n_col):
        ratio += msg[k * n_row : (k + 1) * n_row, :]
    high = ratio.astype(jnp.bfloat16)
    rest = ratio - high.astype(jnp.float32)
    middle = rest.astype(jnp.bfloat16)
    low = (rest - middle.astype(jnp.float32)).astype(jnp.bfloat16)
    found = jnp.zeros((n_row, n_mine), jnp.float32)
    for part in (high, middle, low):
        found += jnp.dot(part, hot[...], preferred_element_type=jnp.float32)
    which = lax.broadcasted_iota(jnp.int32, found.shape, 0)
    out_ref[...] = jnp.sum(jnp.where(which == owner, found, 0.0), axis=0, keepdims=True)
    sum_closed = jnp.sum(ratio[:, n_rows : n_rows + 1], axis=0, keepdims=True)
    sum_wedges = jnp.sum(ratio[:, n_rows + 1 : n_rows + 2], axis=0, keepdims=True)
    total_ref[...] = sum_closed / (sum_wedges * (1.0 / n_col))
    for copy in posts:
        copy.wait_send()


def solution(mesh):
    n_row, n_col = mesh.shape["row"], mesh.shape["col"]
    n_all = n_row * n_col

    def body(adjacency, relabel):
        n_rows, n_words = adjacency.shape
        n_mine = relabel.shape[0]
        depth = 32 * n_words
        every = n_row * n_rows
        width = (n_rows + 2 + 127) // 128 * 128
        clustering, total = pl.pallas_call(
            functools.partial(kernel, n_row, n_col),
            out_shape=(
                jax.ShapeDtypeStruct((1, n_mine), jnp.float32),
                jax.ShapeDtypeStruct((1, 1), jnp.float32),
            ),
            in_specs=[pl.BlockSpec(memory_space=pl.ANY)] * 2,
            out_specs=[pl.BlockSpec(memory_space=pltpu.VMEM)] * 2,
            scratch_shapes=[
                pltpu.VMEM((n_col, n_words, n_rows), jnp.int32),
                pltpu.VMEM((n_row, n_words, n_rows), jnp.int32),
                pltpu.VMEM((n_words, every), jnp.int32),
                pltpu.VMEM((every, n_rows), TYPE),
                pltpu.VMEM((depth + 32, every), TYPE),
                pltpu.VMEM((width, n_mine), jnp.bfloat16),
                pltpu.VMEM((1, n_mine), jnp.int32),
                pltpu.VMEM((n_all, width), jnp.float32),
                pltpu.SemaphoreType.DMA((n_col - 1,)),
                pltpu.SemaphoreType.DMA((n_col,)),
                pltpu.SemaphoreType.DMA((n_row - 1,)),
                pltpu.SemaphoreType.DMA((n_row,)),
                pltpu.SemaphoreType.DMA((n_all - 1,)),
                pltpu.SemaphoreType.DMA((n_all,)),
                pltpu.SemaphoreType.DMA((3,)),
            ],
            compiler_params=pltpu.CompilerParams(
                collective_id=0, has_side_effects=True, vmem_limit_bytes=64000 * 1024
            ),
        )(adjacency.T, relabel.reshape(1, n_mine))
        return clustering.reshape(n_mine), total.reshape(())

    placed = (P("row", "col"), P(("row", "col")))
    return jax.shard_map(
        body, mesh=mesh, in_specs=placed, out_specs=(P(("row", "col")), P()), check_vma=False
    )
```

```python
import functools

import jax
import jax.numpy as jnp
from jax import lax
from jax.experimental import pallas as pl
from jax.experimental.pallas import tpu as pltpu
from jax.sharding import PartitionSpec as P

MESH = pl.DeviceIdType.MESH
TYPE = jnp.float8_e4m3fn


def unpack(row):
    wide = jnp.broadcast_to(row, (32, row.shape[1]))
    bits = lax.shift_right_logical(wide, lax.broadcasted_iota(jnp.int32, wide.shape, 0)) & 1
    return bits.astype(jnp.float32).astype(TYPE)


def kernel(
    n_row, n_col, words_ref, relabel_ref, out_ref, total_ref,
    xs, ys, yw, x, y, hot, rel, msg,
    x_send, x_recv, y_send, y_recv, m_send, m_recv, local_sem,
):
    n_words, n_rows = words_ref.shape
    n_mine = relabel_ref.shape[1]
    depth = 32 * n_words
    width = msg.shape[1]
    r, c = lax.axis_index("row"), lax.axis_index("col")
    barrier = pltpu.get_barrier_semaphore()
    col_peers = [lax.rem(c + o, n_col) for o in range(1, n_col)]
    row_peers = [lax.rem(r + o, n_row) for o in range(1, n_row)]
    for p in col_peers:
        pl.semaphore_signal(barrier, inc=1, device_id=(r, p), device_id_type=MESH)
    for p in row_peers:
        pl.semaphore_signal(barrier, inc=1, device_id=(p, c), device_id_type=MESH)
    load_x = pltpu.make_async_copy(words_ref, xs.at[c], local_sem.at[0])
    load_y = pltpu.make_async_copy(words_ref, ys.at[r], local_sem.at[1])
    load_r = pltpu.make_async_copy(relabel_ref, rel, local_sem.at[2])
    load_x.start()
    load_y.start()
    load_r.start()
    load_x.wait()
    load_y.wait()
    pl.semaphore_wait(barrier, n_col + n_row - 2)

    sends = []
    for i, p in enumerate(col_peers):
        sends.append(pltpu.make_async_remote_copy(
            xs.at[c], xs.at[c], x_send.at[i], x_recv.at[c], device_id=(r, p), device_id_type=MESH))
    for i, p in enumerate(row_peers):
        sends.append(pltpu.make_async_remote_copy(
            ys.at[r], ys.at[r], y_send.at[i], y_recv.at[r], device_id=(p, c), device_id_type=MESH))
    for copy in sends:
        copy.start()

    load_r.wait()
    label = rel[...]
    owner = jnp.zeros_like(label)
    for k in range(1, n_row):
        owner += (label >= k * n_rows).astype(jnp.int32)
    place = label - owner * n_rows
    hot[...] = (lax.broadcasted_iota(jnp.int32, hot.shape, 0) == place).astype(jnp.float32).astype(jnp.bfloat16)
    y[depth:, :] = jnp.ones((y.shape[0] - depth, y.shape[1]), TYPE)

    def take_x(block):
        def one(w, carry):
            start = pl.multiple_of(block * depth + w * 32, 32)
            x[pl.ds(start, 32), :] = unpack(xs[block, pl.ds(w, 1), :])
            return carry
        lax.fori_loop(0, n_words, one, 0, unroll=4)

    take_x(c)
    for i, p in enumerate(col_peers):
        pltpu.make_async_remote_copy(
            xs.at[p], xs.at[p], x_send.at[i], x_recv.at[p], device_id=(r, p), device_id_type=MESH).wait_recv()
        take_x(p)
    for i, p in enumerate(row_peers):
        pltpu.make_async_remote_copy(
            ys.at[p], ys.at[p], y_send.at[i], y_recv.at[p], device_id=(p, c), device_id_type=MESH).wait_recv()
    yw[...] = jnp.concatenate([ys[k] for k in range(n_row)], axis=1)

    def one_y(w, carry):
        y[pl.ds(pl.multiple_of(w * 32, 32), 32), :] = unpack(yw[pl.ds(w, 1), :])
        return carry
    lax.fori_loop(0, n_words, one_y, 0, unroll=2)

    paths = jnp.dot(y[...], x[...], preferred_element_type=jnp.float32)
    mask = x[pl.ds(pl.multiple_of(c * depth, 32), depth), :].astype(jnp.float32)
    closed = jnp.sum(paths[:depth] * mask, axis=0, keepdims=True)
    degree = paths[depth : depth + 1]
    wedges = jnp.maximum(degree * (degree - 1.0), 1.0)
    sums = lax.broadcasted_iota(jnp.int32, (1, width - n_rows), 1)
    tail = jnp.where(sums == 0, jnp.sum(closed), jnp.where(sums == 1, jnp.sum(wedges), 0.0))
    me = c * n_row + r
    msg[pl.ds(me, 1), :] = jnp.concatenate([closed / wedges, tail], axis=1)

    posts = []
    for i in range(n_row * n_col - 1):
        to = i + (i >= me).astype(jnp.int32)
        posts.append(pltpu.make_async_remote_copy(
            msg.at[pl.ds(me, 1)], msg.at[pl.ds(me, 1)], m_send.at[i], m_recv.at[me],
            device_id=(lax.rem(to, n_row), to // n_row), device_id_type=MESH))
    for copy in posts:
        copy.start()
    for copy in sends:
        copy.wait_send()
    for o in range(1, n_row * n_col):
        p = lax.rem(me + o, n_row * n_col)
        pltpu.make_async_copy(msg.at[pl.ds(p, 1)], msg.at[pl.ds(p, 1)], m_recv.at[p]).wait()

    ratio = msg[0:n_row, :]
    for k in range(1, n_col):
        ratio += msg[k * n_row : (k + 1) * n_row, :]
    high = ratio.astype(jnp.bfloat16)
    rest = ratio - high.astype(jnp.float32)
    middle = rest.astype(jnp.bfloat16)
    low = (rest - middle.astype(jnp.float32)).astype(jnp.bfloat16)
    parts = jnp.concatenate([p.astype(jnp.float32) for p in (high, middle, low)], axis=0).astype(jnp.bfloat16)
    picked = jnp.dot(parts, hot[...], preferred_element_type=jnp.float32)
    found = picked[:n_row] + picked[n_row : 2 * n_row] + picked[2 * n_row :]
    which = lax.broadcasted_iota(jnp.int32, found.shape, 0)
    out_ref[...] = jnp.sum(jnp.where(which == owner, found, 0.0), axis=0, keepdims=True)
    sum_closed = jnp.sum(ratio[:, n_rows : n_rows + 1], axis=0, keepdims=True)
    sum_wedges = jnp.sum(ratio[:, n_rows + 1 : n_rows + 2], axis=0, keepdims=True)
    total_ref[...] = sum_closed / (sum_wedges * (1.0 / n_col))
    for copy in posts:
        copy.wait_send()


def solution(mesh):
    n_row, n_col = mesh.shape["row"], mesh.shape["col"]
    n_all = n_row * n_col

    def body(adjacency, relabel):
        n_rows, n_words = adjacency.shape
        n_mine = relabel.shape[0]
        depth = 32 * n_words
        every = n_row * n_rows
        width = (n_rows + 2 + 127) // 128 * 128
        clustering, total = pl.pallas_call(
            functools.partial(kernel, n_row, n_col),
            out_shape=(
                jax.ShapeDtypeStruct((1, n_mine), jnp.float32),
                jax.ShapeDtypeStruct((1, 1), jnp.float32),
            ),
            in_specs=[pl.BlockSpec(memory_space=pl.ANY)] * 2,
            out_specs=[pl.BlockSpec(memory_space=pltpu.VMEM)] * 2,
            scratch_shapes=[
                pltpu.VMEM((n_col, n_words, n_rows), jnp.int32),
                pltpu.VMEM((n_row, n_words, n_rows), jnp.int32),
                pltpu.VMEM((n_words, every), jnp.int32),
                pltpu.VMEM((every, n_rows), TYPE),
                pltpu.VMEM((depth + 32, every), TYPE),
                pltpu.VMEM((width, n_mine), jnp.bfloat16),
                pltpu.VMEM((1, n_mine), jnp.int32),
                pltpu.VMEM((n_all, width), jnp.float32),
                pltpu.SemaphoreType.DMA((n_col - 1,)),
                pltpu.SemaphoreType.DMA((n_col,)),
                pltpu.SemaphoreType.DMA((n_row - 1,)),
                pltpu.SemaphoreType.DMA((n_row,)),
                pltpu.SemaphoreType.DMA((n_all - 1,)),
                pltpu.SemaphoreType.DMA((n_all,)),
                pltpu.SemaphoreType.DMA((3,)),
            ],
            compiler_params=pltpu.CompilerParams(
                collective_id=0, has_side_effects=True, vmem_limit_bytes=64000 * 1024
            ),
        )(adjacency.T, relabel.reshape(1, n_mine))
        return clustering.reshape(n_mine), total.reshape(())

    placed = (P("row", "col"), P(("row", "col")))
    return jax.shard_map(
        body, mesh=mesh, in_specs=placed, out_specs=(P(("row", "col")), P()), check_vma=False
    )
```
